256 devices in a mesh: rep: 32 (over x, z_lo, core), fsdp: 8 (over z_hi, y).
Axes of the slice: x: 4, y: 4, z: 8 (z_hi: 2, z_lo: 4; z = z_hi * 4 + z_lo), core: 2. Of those that a mesh axis runs over, the one named last changes fastest.
Arguments:
- hidden: bfloat16 [32768, 8192], P(('rep', 'fsdp')), may hold values from -6 to 6
- local_weight: bfloat16 [32, 8192, 2048], P('rep', 'fsdp'), may hold values from -0.125 to 0.125
- master: float32 [8192, 2048], P('fsdp', 'rep'), may hold values from -0.0625 to 0.0625
- momentum: float32 [8192, 2048], P('fsdp', 'rep'), may hold values from -0.06 to 0.06
- dither: int32 [32, 8192, 16], P('rep', 'fsdp'), may hold values from 0 to 15
Outputs:
- key_values: bfloat16 [32768, 2048], P(('rep', 'fsdp'))
- new_master: float32 [8192, 2048], P('fsdp', 'rep')
- new_momentum: float32 [8192, 2048], P('fsdp', 'rep')
- new_local: bfloat16 [32, 8192, 2048], P('rep', 'fsdp')
The draws below stay inside these ranges and needn't reach their ends.
All inputs are finite; a program needn't handle non-finite values.
Results may differ from the reference program's by a relative error of at most 0.0067.
Values may be sent and summed in bfloat16 or wider, within the bound.
A program may use at most 192 MiB of HBM per device.

```python
import math
import jax
import jax.numpy as jnp
from jax import lax

D = 8192
BLOCK = 128
KVW = 2048
TOKENS = 32768
N_REP = 32


def place_ends(array, rng, smallest, largest):
    place = [jax.random.randint(jax.random.fold_in(rng, axis), (), 0, length) for axis, length in enumerate(array.shape)]
    widest = array.shape.index(max(array.shape))
    beside = place[:widest] + [(place[widest] + 1) % array.shape[widest]] + place[widest + 1:]
    return array.at[tuple(place)].set(smallest).at[tuple(beside)].set(largest)


def strengthened(drawn, stream_key, source, target, blocks, factor):
    def block_of(dim):
        return (jnp.arange(drawn.shape[dim]) // (drawn.shape[dim] // blocks)).reshape((-1,) + (1,) * (drawn.ndim - 1 - dim))

    first = jax.random.permutation(stream_key, blocks)[block_of(target)]
    second = (block_of(target) + blocks // 2) % blocks
    return jnp.where((block_of(source) == first) | (block_of(source) == second), factor * drawn, drawn)


def shard_levels(key, extent, split, least, largest):
    def one(dim, shards_of):
        draws = jax.random.uniform(jax.random.fold_in(jax.random.fold_in(key, 6), dim), (shards_of,), jnp.float32, least / len(split), largest / len(split))
        return jnp.repeat(jnp.exp(draws), extent[dim] // shards_of).reshape((-1,) + (1,) * (len(extent) - dim - 1))

    level = one(*split[0])
    for cut in split[1:]:
        level = level * one(*cut)
    return level


def centred(own_key, shape, deviation, most, cuts=(), held_as=jnp.bfloat16):
    array = deviation * jax.random.normal(own_key, shape, jnp.float32)
    if cuts:
        array = array * shard_levels(own_key, shape, cuts, -0.22, 0.18)
    return jnp.clip(array, -most, most).astype(held_as)


def bell_draw_with(stream_key, extent, spread, reach, pieces, heavy, dtype=jnp.bfloat16):
    values = spread * jax.random.normal(stream_key, extent, jnp.float32)
    if pieces:
        values = values * shard_levels(stream_key, extent, pieces, -0.22, 0.18)
    return jnp.clip(strengthened(values, jax.random.fold_in(stream_key, 3), *heavy), -reach, reach).astype(dtype)


def setup_inputs(seed: int = 0) -> dict:
    key_list = jax.random.split(jax.random.key(seed), 6)
    return {
        "hidden": centred(key_list[0], (TOKENS, D), 1.0, 6.0, ((0, 256),)),
        "local_weight": bell_draw_with(key_list[1], (N_REP, D, KVW), D ** -0.5, 0.125, ((0, 32), (1, 8)), (0, 2, 32, 2.75)),
        "master": centred(key_list[2], (D, KVW), D ** -0.5, 0.0625, ((0, 8), (1, 32)), jnp.float32),
        "momentum": centred(key_list[3], (D, KVW), 0.01, 0.06, ((0, 8), (1, 32)), jnp.float32),
        "dither": place_ends(jax.random.randint(key_list[4], (N_REP, D, KVW // BLOCK), 0, 16), jax.random.fold_in(key_list[4], 1), 0, 15).astype(jnp.int32),
    }


momentum_keep = 0.9
outer_rate = 0.7
mix_share = 0.5


def code_block(delta, dither):
    row_count = delta.shape[0]
    blocked = delta.reshape(row_count, -1, BLOCK)
    scaling = (jnp.max(jnp.abs(blocked), axis=2, keepdims=True) + 1e-6) / 7.0
    offset = (dither.astype(jnp.float32)[:, :, None] + 0.5) / 16.0 - 0.5
    levels = jnp.clip(blocked / scaling + offset, -8.0, 7.0)
    smooth = levels - jnp.sin(2.0 * math.pi * levels) / (2.0 * math.pi)
    return (scaling * (smooth - offset)).reshape(row_count, -1)


def reference(hidden, local_weight, master, momentum, dither):
    anchor = lax.optimization_barrier(master.astype(jnp.bfloat16)).astype(jnp.float32)

    def accumulate(summed, pair_items):
        weights, offsets = pair_items
        coded = code_block(anchor - weights.astype(jnp.float32), offsets).astype(jnp.bfloat16)
        return summed + lax.optimization_barrier(coded).astype(jnp.float32), None

    summed, _ = lax.scan(accumulate, jnp.zeros(master.shape, jnp.float32), (local_weight, dither))
    averaged = summed / N_REP
    new_momentum = momentum_keep * momentum + averaged
    new_master = master - outer_rate * (averaged + momentum_keep * new_momentum)
    rounded = lax.optimization_barrier(new_master.astype(jnp.bfloat16)).astype(jnp.float32)

    def merge_one(weights):
        return (mix_share * weights.astype(jnp.float32) + (1.0 - mix_share) * rounded).astype(jnp.bfloat16)

    new_local = lax.map(merge_one, local_weight)
    grouped = hidden.reshape(N_REP, -1, D)

    def project(pair_items):
        return jnp.dot(pair_items[0], pair_items[1], preferred_element_type=jnp.float32).astype(jnp.bfloat16)

    key_values = lax.map(project, (grouped, local_weight)).reshape(-1, KVW)
    return key_values, new_master, new_momentum, new_local
```

```python
import functools

import jax
import jax.numpy as jnp
from jax import lax
from jax.experimental import pallas as pl
from jax.experimental.pallas import tpu as pltpu
from jax.sharding import Mesh
from jax.sharding import PartitionSpec as P

BLOCK = 128
FSDP = ("zh", "y")
REP = ("x", "z", "c")
REP_FSDP = ("x", "z", "c", "zh", "y")
MESH = pl.DeviceIdType.MESH

momentum_keep = 0.9
outer_rate = 0.7
mix_share = 0.5

NC = 2
F32 = jnp.float32
BF16 = jnp.bfloat16

SINC = (0.9999999993, -6.579735975, 12.98786004, -12.20766404, 6.688634018, -2.371384249, 0.5153655921)


def sine_share(levels):
    turn = levels - jnp.round(levels)
    square = turn * turn
    series = jnp.full_like(square, SINC[-1])
    for coefficient in SINC[-2::-1]:
        series = series * square + coefficient
    return turn * series


def kernel(
    hidden, weights, dither, master, momentum,
    key_values, new_master, new_momentum, new_local,
    wv, dv, mas, mom, mas_in, mom_in, nmas, nmom, held, coded, paired, rx1, rx2, rz, fresh, merged,
    hr, ps1, pr1, ps2, pr2, psz, prz, kept, kv,
    send_sem, recv_sem, local_sem,
):
    rows, columns = wv.shape
    blocks = columns // BLOCK
    groups, _, rc, _ = held.shape
    x, z, c = lax.axis_index("x"), lax.axis_index("z"), lax.axis_index("c")
    zh, y = lax.axis_index("zh"), lax.axis_index("y")

    def flips(i):
        return i, i + 1 - 2 * lax.rem(i, 2), lax.rem(i + 2, 4), 3 - i

    xs, zs, ys = flips(x), flips(z), flips(y)
    x1, x3 = xs[1], xs[3]
    mine = x * 4 + z
    pair = lax.div(x, 2)

    counts = {"remote": 0, "local": 0}
    sends = []
    puts = []

    def remote(src, dst, target):
        i = counts["remote"]
        counts["remote"] += 1
        copy = pltpu.make_async_remote_copy(
            src_ref=src, dst_ref=dst, send_sem=send_sem.at[i], recv_sem=recv_sem.at[i],
            device_id=target, device_id_type=MESH,
        )
        copy.start()
        sends.append(copy)
        return copy

    def local(src, dst):
        i = counts["local"]
        counts["local"] += 1
        copy = pltpu.make_async_copy(src, dst, local_sem.at[i])
        copy.start()
        return copy

    in_master = local(master, mas)
    in_weights = local(weights, wv)
    in_dither = local(dither, dv)
    in_momentum = local(momentum, mom)
    depth = hr.shape[3]
    own_columns = pl.ds(pl.multiple_of((zh * 4 + y) * depth, depth), depth)
    in_hidden = local(hidden.at[:, own_columns], hr.at[0, 0])

    barrier = pltpu.get_barrier_semaphore()
    peers = [{"c": 1 - c}, {"x": x1}, {"x": x3}]
    peers += [{"z": zs[d]} for d in (1, 2, 3)]
    peers += [{"y": ys[d]} for d in (1, 2, 3)]
    peers += [{"zh": 1 - zh, "y": ys[d]} for d in range(4)]
    for peer in peers:
        pl.semaphore_signal(barrier, inc=1, device_id=peer, device_id_type=MESH)
    pl.semaphore_wait(barrier, len(peers))

    half_rows = rows // 2
    my_rows = pl.ds(pl.multiple_of(c * half_rows, half_rows), half_rows)
    other_rows = pl.ds(pl.multiple_of((1 - c) * half_rows, half_rows), half_rows)
    in_master.wait()
    got_master = remote(mas.at[other_rows], mas_in, {"c": 1 - c})

    def first_group(half, k):
        return (half * NC + k) * 2

    def group_rows(group):
        return pl.multiple_of(group * rc, rc)

    def gather_start(buffer, k):
        g = first_group(c, k)
        piece = buffer.at[pl.ds(g, 2), mine]
        over_z = [remote(piece, piece, {"z": zs[d]}) for d in (1, 2, 3)]
        return over_z

    def gather(buffer, k, over_z, times):
        g = first_group(c, k)
        partner = {"c": 1 - c}

        def pass_on(part):
            return remote(part, part, partner)

        def part(ab, first, count):
            return buffer.at[g + ab, pl.ds(first, count)]

        yield times[0]
        for copy in over_z:
            copy.wait_recv()
        own_a, own_b = part(0, 4 * x, 4), part(1, 4 * x, 4)
        a1 = remote(own_a, own_a, {"x": x1})
        b1 = remote(own_b, own_b, {"x": x3})
        b2 = remote(own_b, own_b, {"x": x1})
        a2 = remote(own_a, own_a, {"x": x3})
        passed = [pass_on(buffer.at[pl.ds(g, 2), pl.ds(4 * x, 4)])]
        yield times[1]
        a1.wait_recv()
        far_a = part(0, 4 * x1, 4)
        a3 = remote(far_a, far_a, {"x": x3})
        passed.append(pass_on(far_a))
        b1.wait_recv()
        far_b = part(1, 4 * x3, 4)
        b3 = remote(far_b, far_b, {"x": x1})
        passed.append(pass_on(far_b))
        yield times[2]
        b2.wait_recv()
        passed.append(pass_on(part(1, 4 * x1, 4)))
        a2.wait_recv()
        passed.append(pass_on(part(0, 4 * x3, 4)))
        a3.wait_recv()
        passed.append(pass_on(part(0, 4 * xs[2], 4)))
        b3.wait_recv()
        passed.append(pass_on(part(1, 4 * xs[2], 4)))
        yield times[3]
        for copy in passed:
            copy.wait_recv()

    tile = 16

    def code_groups(first, count):
        start = group_rows(first)

        @pl.loop(0, count * rc // tile)
        def _(i):
            at = pl.multiple_of(start + i * tile, tile)
            group = first + lax.div(i, rc // tile)
            inner = pl.multiple_of(lax.rem(i, rc // tile) * tile, tile)
            here = pl.ds(inner, tile)
            offsets = (dv[pl.ds(at, tile), :].astype(F32) + 0.5) / 16.0 - 0.5
            for b in range(blocks):
                old = wv[pl.ds(at, tile), b * BLOCK:(b + 1) * BLOCK].astype(F32)
                delta = held[group, b, here, :].astype(F32) - old
                largest = jnp.max(jnp.abs(delta), axis=1, keepdims=True)
                scaling = (largest + 1e-06) / 7.0
                offset = offsets[:, b:b + 1]
                levels = jnp.clip(delta * (1.0 / scaling) + offset, -8.0, 7.0)
                smooth = levels - sine_share(levels)
                coded[group, b, here, :] = (scaling * (smooth - offset)).astype(BF16)

    def add_into(target, source):
        step = 64 if rc % 64 == 0 else rc
        n = source.shape[0]

        @pl.loop(0, n * (rc // step))
        def _(i):
            at = (lax.div(i, rc // step), pl.ds(pl.multiple_of(lax.rem(i, rc // step) * step, step), step))
            target[at] = (target[at].astype(F32) + source[at].astype(F32)).astype(BF16)

    def chunk(k, times):
        g, other = first_group(c, k), first_group(1 - c, k)
        times = iter(times)
        yield from gather(held, k, anchors[k], [next(times) for _ in range(4)])
        code_groups(other, 2)
        got = remote(coded.at[pl.ds(other, 2)], paired.at[k], {"c": 1 - c})
        code_groups(g, 2)
        yield next(times)
        got.wait_recv()
        ga, gb = g, g + 1

        def spot(group, first, count):
            return coded.at[group, pl.ds(first, count)]

        def take(ab, first, count):
            add_into(spot(g + ab, first, count), paired.at[k, ab, pl.ds(first, count)])

        away = 8 * (1 - pair)
        take(0, away, 8)
        a1 = remote(spot(ga, away, 8), rx1.at[k, 0], {"x": x3})
        take(1, 4 * x1, 4)
        b1 = remote(spot(gb, 4 * x1, 4), rx1.at[k, 1, pl.ds(0, 4)], {"x": x1})
        take(1, 4 * xs[2], 4)
        b2 = remote(spot(gb, 4 * xs[2], 4), rx1.at[k, 1, pl.ds(4, 4)], {"x": x1})
        take(0, 8 * pair, 8)
        take(1, 4 * x, 4)
        take(1, 4 * x3, 4)
        yield next(times)
        a1.wait_recv()
        add_into(spot(ga, 4 * x1, 4), rx1.at[k, 0, pl.ds(4 * lax.rem(x1, 2), 4)])
        a3 = remote(spot(ga, 4 * x1, 4), rx2.at[k, 0], {"x": x1})
        b2.wait_recv()
        add_into(spot(gb, 4 * x3, 4), rx1.at[k, 1, pl.ds(4, 4)])
        b3 = remote(spot(gb, 4 * x3, 4), rx2.at[k, 1], {"x": x3})
        add_into(spot(ga, 4 * x, 4), rx1.at[k, 0, pl.ds(4 * lax.rem(x, 2), 4)])
        b1.wait_recv()
        add_into(spot(gb, 4 * x, 4), rx1.at[k, 1, pl.ds(0, 4)])
        yield next(times)
        a3.wait_recv()
        add_into(spot(ga, 4 * x, 4), rx2.at[k, 0])
        b3.wait_recv()
        add_into(spot(gb, 4 * x, 4), rx2.at[k, 1])
        over_z = [
            remote(coded.at[pl.ds(g, 2), 4 * x + zs[d]], rz.at[k, d - 1], {"z": zs[d]}) for d in (1, 2, 3)
        ]
        yield next(times)
        for copy in over_z:
            copy.wait_recv()
        if k == 0:
            got_momentum.wait_recv()
        replicas = 32.0
        for ab in range(2):
            summed = coded[g + ab, mine].astype(F32)
            for d in range(3):
                summed = summed + rz[k, d, ab].astype(F32)
            averaged = summed / replicas
            all_rows = pl.ds(group_rows(g + ab), rc)
            half_at = pl.ds((k * 2 + ab) * rc, rc)
            moved = momentum_keep * (mom[all_rows] + mom_in[half_at]) + averaged
            stepped = mas_in[half_at] - outer_rate * (averaged + momentum_keep * moved)
            nmom[all_rows] = moved
            nmas[all_rows] = stepped
            fresh[g + ab, mine] = stepped.astype(BF16)
        news = gather_start(fresh, k)
        chunk_rows = pl.ds(group_rows(g), 2 * rc)
        got_nmas = remote(nmas.at[chunk_rows], nmas.at[chunk_rows], {"c": 1 - c})
        got_nmom = remote(nmom.at[chunk_rows], nmom.at[chunk_rows], {"c": 1 - c})
        yield from gather(fresh, k, news, [next(times) for _ in range(4)])
        for first in (g, other):
            start = group_rows(first)

            @pl.loop(0, 2 * rc // tile)
            def _(i):
                at = pl.multiple_of(start + i * tile, tile)
                group = first + lax.div(i, rc // tile)
                here = pl.ds(pl.multiple_of(lax.rem(i, rc // tile) * tile, tile), tile)
                for b in range(blocks):
                    lanes = slice(b * BLOCK, (b + 1) * BLOCK)
                    old = wv[pl.ds(at, tile), lanes].astype(F32)
                    new = fresh[group, b, here, :].astype(F32)
                    merged[pl.ds(at, tile), lanes] = (mix_share * old + (1.0 - mix_share) * new).astype(BF16)

            span = pl.ds(start, 2 * rc)
            puts.append(local(merged.at[span], new_local.at[span]))
        yield next(times)
        got_nmas.wait_recv()
        got_nmom.wait_recv()
        for first in (g, other):
            span = pl.ds(group_rows(first), 2 * rc)
            puts.append(local(nmas.at[span], new_master.at[span]))
            puts.append(local(nmom.at[span], new_momentum.at[span]))

    def hidden_sends(dz):
        copies = {}
        for d in (2, 1, 3, 0):
            if dz == 0 and d == 0:
                continue
            to_z = (1 - zh) if dz else zh
            span = pl.ds(pl.multiple_of((to_z * 4 + ys[d]) * depth, depth), depth)
            target = {"zh": to_z, "y": ys[d]} if dz else {"y": ys[d]}
            copies[d] = remote(hidden.at[:, span], hr.at[dz, d], target)
        return copies

    half_columns = columns // 2
    step = 256
    tokens = hr.shape[2]

    def product(dz, d, count, side, write):
        left = hr[dz, pl.ds(d, count)].reshape(count * tokens, depth)

        @pl.loop(0, half_columns // step)
        def _(i):
            at = pl.multiple_of(i * step, step)
            right = wv[:, pl.ds(pl.multiple_of(side * half_columns + at, step), step)]
            write(pl.ds(at, step), jnp.dot(left, right, preferred_element_type=F32))

    def project(dz, arrived, times):
        times = iter(times)
        yield next(times)
        if dz == 0:
            in_hidden.wait()
        for d in (2, 1, 3, 0):
            if d in arrived:
                arrived[d].wait_recv()

        def store(side):
            def write(at, value):
                ps1[dz, side, :, :, at] = value.reshape(2, tokens, step).astype(BF16)
            return write

        product(dz, 1, 2, 0, store(0))
        left1 = remote(ps1.at[dz, 0], pr1.at[dz, 0], {"y": ys[1]})
        product(dz, 2, 2, 1, store(1))
        right1 = remote(ps1.at[dz, 1], pr1.at[dz, 1], {"y": ys[3]})

        yield next(times)

        def joined(side, slot):
            def write(at, value):
                ps2[dz, side, :, at] = (value + pr1[dz, side, slot, :, at].astype(F32)).astype(BF16)
            return write

        left1.wait_recv()
        product(dz, 3, 1, 0, joined(0, 1))
        left2 = remote(ps2.at[dz, 0], pr2.at[dz, 0], {"y": ys[3]})
        right1.wait_recv()
        product(dz, 1, 1, 1, joined(1, 0))
        right2 = remote(ps2.at[dz, 1], pr2.at[dz, 1], {"y": ys[1]})

        def keep(side, slot):
            def write(at, value):
                kept[dz, side, :, at] = value + pr1[dz, side, slot, :, at].astype(F32)
            return write

        product(dz, 0, 1, 0, keep(0, 0))
        product(dz, 0, 1, 1, keep(1, 1))
        yield next(times)
        left2.wait_recv()
        right2.wait_recv()
        if dz == 1:
            for side in range(2):
                psz[side] = (kept[1, side] + pr2[1, side].astype(F32)).astype(BF16)
            crossed = remote(psz, prz, {"zh": 1 - zh})
            yield next(times)
            crossed.wait_recv()
            for side in range(2):
                total = kept[0, side] + pr2[0, side].astype(F32) + prz[side].astype(F32)
                kv[:, side * half_columns:(side + 1) * half_columns] = total.astype(BF16)
            puts.append(local(kv, key_values))

    in_momentum.wait()
    got_momentum = remote(mom.at[other_rows], mom_in, {"c": 1 - c})
    got_master.wait_recv()
    mas_in[...] = mas_in[...] + mas[my_rows]
    for k in range(NC):
        for ab in range(2):
            held[first_group(c, k) + ab, mine] = mas_in[(k * 2 + ab) * rc:(k * 2 + ab + 1) * rc].astype(BF16)
    anchors = [gather_start(held, k) for k in range(NC)]
    crossing = hidden_sends(1)
    beside = hidden_sends(0)
    in_weights.wait()
    in_dither.wait()

    runs = [chunk(k, CHUNK_TIMES[k]) for k in range(NC)]
    runs += [project(0, beside, NEAR_TIMES), project(1, crossing, FAR_TIMES)]
    due = [(next(run), i, run) for i, run in enumerate(runs)]
    while due:
        due.sort(key=lambda entry: entry[:2])
        _, i, run = due.pop(0)
        when = next(run, None)
        if when is not None:
            due.append((when, i, run))
    for copy in sends:
        copy.wait_send()
    for copy in puts:
        copy.wait()


CHUNK_TIMES = [
    [12, 16, 23, 25, 33, 42, 47, 54, 61, 66, 73, 75, 76],
    [18, 24, 32, 36, 46, 56, 61, 69, 76, 81, 88, 90, 91],
]
NEAR_TIMES = [30, 44, 52]
FAR_TIMES = [58, 72, 78, 101]


def shards(hidden, local_weight, master, momentum, dither):
    weights = local_weight[0]
    rows, columns = weights.shape
    tokens, width = hidden.shape
    lanes = master.shape[1]
    core = lax.axis_index("c")
    blocks = columns // BLOCK
    groups = 4 * NC
    rc = rows // groups
    depth = width // 8

    def widened(part):
        low = jnp.pad(part, ((0, 0), (0, lanes)))
        high = jnp.pad(part, ((0, 0), (lanes, 0)))
        return jnp.where(core == 0, low, high)

    def narrowed(part):
        return jnp.where(core == 0, part[:, :lanes], part[:, lanes:])

    hbm = pl.BlockSpec(memory_space=pl.ANY)
    vm = pltpu.VMEM
    half = columns // 2
    scratch = [
        vm((rows, columns), BF16),
        vm((rows, blocks), jnp.int32),
        vm((rows, BLOCK), F32),
        vm((rows, BLOCK), F32),
        vm((rows // 2, BLOCK), F32),
        vm((rows // 2, BLOCK), F32),
        vm((rows, BLOCK), F32),
        vm((rows, BLOCK), F32),
        vm((groups, blocks, rc, BLOCK), BF16),
        vm((groups, blocks, rc, BLOCK), BF16),
        vm((NC, 2, blocks, rc, BLOCK), BF16),
        vm((NC, 2, 8, rc, BLOCK), BF16),
        vm((NC, 2, 4, rc, BLOCK), BF16),
        vm((NC, 3, 2, rc, BLOCK), BF16),
        vm((groups, blocks, rc, BLOCK), BF16),
        vm((rows, columns), BF16),
        vm((2, 4, tokens, depth), BF16),
        vm((2, 2, 2, tokens, half), BF16),
        vm((2, 2, 2, tokens, half), BF16),
        vm((2, 2, tokens, half), BF16),
        vm((2, 2, tokens, half), BF16),
        vm((2, tokens, half), BF16),
        vm((2, tokens, half), BF16),
        vm((2, 2, tokens, half), F32),
        vm((tokens, columns), BF16),
        pltpu.SemaphoreType.DMA((24 + 48 * NC,)),
        pltpu.SemaphoreType.DMA((24 + 48 * NC,)),
        pltpu.SemaphoreType.DMA((8 + 8 * NC,)),
    ]
    key_values, wide_master, wide_momentum, new_local = pl.pallas_call(
        kernel,
        out_shape=(
            jax.ShapeDtypeStruct((tokens, columns), BF16),
            jax.ShapeDtypeStruct((rows, BLOCK), F32),
            jax.ShapeDtypeStruct((rows, BLOCK), F32),
            jax.ShapeDtypeStruct((rows, columns), BF16),
        ),
        in_specs=[hbm] * 5,
        out_specs=[hbm] * 4,
        scratch_shapes=scratch,
        compiler_params=pltpu.CompilerParams(
            collective_id=0, has_side_effects=True, vmem_limit_bytes=60 * 1024 * 1024
        ),
        name="outer_step",
    )(hidden, weights, dither[0], widened(master), widened(momentum))
    return key_values, narrowed(wide_master), narrowed(wide_momentum), new_local[None]


def solution(mesh):
    finer = Mesh(mesh.devices.reshape(4, 4, 2, 2, 4), REP_FSDP)
    in_specs = (P(REP_FSDP, None), P(REP, FSDP, None), P(FSDP, REP), P(FSDP, REP), P(REP, FSDP, None))
    out_specs = (P(REP_FSDP, None), P(FSDP, REP), P(FSDP, REP), P(REP, FSDP, None))
    return jax.shard_map(shards, mesh=finer, in_specs=in_specs, out_specs=out_specs, check_vma=False)
```

```python
import functools

import jax
import jax.numpy as jnp
from jax import lax
from jax.experimental import pallas as pl
from jax.experimental.pallas import tpu as pltpu
from jax.sharding import Mesh
from jax.sharding import PartitionSpec as P

BLOCK = 128
FSDP = ("zh", "y")
REP = ("x", "z", "c")
REP_FSDP = ("x", "z", "c", "zh", "y")
MESH = pl.DeviceIdType.MESH

momentum_keep = 0.9
outer_rate = 0.7
mix_share = 0.5

NC = 4
FAR = 2
SUB = 2
RET = 4
ORDER = [-1, -1, 0, -1, 1, 0, 0, 4, -1, 2, 1, 1, -1, 3, 0, -1, 0, -1, 1, -1, 2, 0, 1, -1, 2, 3, 3, 4, 4, -1, 1, 0, 2, -1, 2, -1, 1, 3, -1, 0, 2, 3, 1, 4, 5, 3, 2, -1, -1, 3, -1, 5, 2, 5, 3, 0, 1, 5, -1, -1, 2, 6, 3, 0, -1, 1, 6, 0, 0, -1, 6, 1, 1, 0, 6, -1, -1, 2, 1, 0, 0, -1, 1, 1, 3, 2, 2, -1, 3, 3, 2, 5, 3, 2, 2, 3, 3, 6]
F32 = jnp.float32
BF16 = jnp.bfloat16

SINC = (0.9999999993, -6.579735975, 12.98786004, -12.20766404, 6.688634018, -2.371384249, 0.5153655921)


def sine_share(levels):
    turn = levels - jnp.round(levels)
    square = turn * turn
    series = jnp.full_like(square, SINC[-1])
    for coefficient in SINC[-2::-1]:
        series = series * square + coefficient
    return turn * series


def kernel(
    hidden, weights, dither, master, momentum,
    key_values, new_master, new_momentum, new_local,
    wv, dv, narrow, offsets, mas_t, mom_t, mas, mom, turned,
    held, coded, paired, rx1, rx2, rz, fresh,
    hr, ps1, pr1, ps2, pr2, psz, prz, kept,
    send_sem, recv_sem, local_sem,
):
    rows, columns = wv.shape
    blocks = columns // BLOCK
    lanes = BLOCK // 2
    groups, _, rc, _ = held.shape
    x, z, c = lax.axis_index("x"), lax.axis_index("z"), lax.axis_index("c")
    zh, y = lax.axis_index("zh"), lax.axis_index("y")

    def flips(i):
        return i, i + 1 - 2 * lax.rem(i, 2), lax.rem(i + 2, 4), 3 - i

    xs, zs, ys = flips(x), flips(z), flips(y)
    x1, x3 = xs[1], xs[3]
    mine = x * 4 + z
    pair = lax.div(x, 2)
    partner = {"c": 1 - c}

    counts = {"remote": 0, "local": 0}
    sends = []
    finished = []

    def remote(src, dst, target):
        i = counts["remote"]
        counts["remote"] += 1
        copy = pltpu.make_async_remote_copy(
            src_ref=src, dst_ref=dst, send_sem=send_sem.at[i], recv_sem=recv_sem.at[i],
            device_id=target, device_id_type=MESH,
        )
        copy.start()
        sends.append(copy)
        return copy

    def local(src, dst):
        i = counts["local"]
        counts["local"] += 1
        copy = pltpu.make_async_copy(src, dst, local_sem.at[i])
        copy.start()
        return copy

    half_rows = rows // 2
    my_rows = pl.ds(pl.multiple_of(c * half_rows, half_rows), half_rows)
    other_rows = pl.ds(pl.multiple_of((1 - c) * half_rows, half_rows), half_rows)
    my_lanes = pl.ds(pl.multiple_of(c * lanes, lanes), lanes)
    depth = hr.shape[3]
    tokens = hr.shape[2]
    in_master = local(master.at[:, my_rows], mas_t.at[my_lanes])
    in_dither = local(dither, dv)
    in_weights = local(weights, wv)
    in_momentum = local(momentum.at[:, my_rows], mom_t.at[my_lanes])
    own_columns = pl.ds(pl.multiple_of((zh * 4 + y) * depth, depth), depth)
    in_hidden = local(hidden.at[:, own_columns], hr.at[0, 0])

    barrier = pltpu.get_barrier_semaphore()
    peers = [partner, {"x": x1}, {"x": x3}]
    peers += [{"z": zs[d]} for d in (1, 2, 3)]
    peers += [{"y": ys[d]} for d in (1, 2, 3)]
    peers += [{"zh": 1 - zh, "y": ys[d]} for d in range(4)]
    for peer in peers:
        pl.semaphore_signal(barrier, inc=1, device_id=peer, device_id_type=MESH)
    pl.semaphore_wait(barrier, len(peers))

    got_master = remote(master.at[:, other_rows], mas_t.at[my_lanes], partner)
    got_momentum = remote(momentum.at[:, other_rows], mom_t.at[my_lanes], partner)

    def first_group(half, k):
        return (half * NC + k) * 2

    def group_rows(group):
        return pl.multiple_of(group * rc, rc)

    def gather_start(buffer, k):
        piece = buffer.at[pl.ds(first_group(c, k), 2), mine]
        return [remote(piece, piece, {"z": zs[d]}) for d in (1, 2, 3)]

    def gather(buffer, k, over_z, between=None):
        g = first_group(c, k)

        def pass_on(part):
            return remote(part, part, partner)

        def part(ab, first, count):
            return buffer.at[g + ab, pl.ds(first, count)]

        yield
        for copy in over_z:
            copy.wait_recv()
        own_a, own_b = part(0, 4 * x, 4), part(1, 4 * x, 4)
        a1 = remote(own_a, own_a, {"x": x1})
        b1 = remote(own_b, own_b, {"x": x3})
        b2 = remote(own_b, own_b, {"x": x1})
        a2 = remote(own_a, own_a, {"x": x3})
        passed = [pass_on(buffer.at[pl.ds(g, 2), pl.ds(4 * x, 4)])]
        yield
        a1.wait_recv()
        far_a = part(0, 4 * x1, 4)
        a3 = remote(far_a, far_a, {"x": x3})
        passed.append(pass_on(far_a))
        yield
        b1.wait_recv()
        far_b = part(1, 4 * x3, 4)
        b3 = remote(far_b, far_b, {"x": x1})
        passed.append(pass_on(far_b))
        yield
        a2.wait_recv()
        a3.wait_recv()
        passed.append(pass_on(part(0, 8 * (1 - pair), 8)))
        b2.wait_recv()
        passed.append(pass_on(part(1, 4 * x1, 4)))
        b3.wait_recv()
        passed.append(pass_on(part(1, 4 * xs[2], 4)))
        if between is not None:
            between()
        yield
        for copy in passed:
            copy.wait_recv()

    tile = 16

    def code_groups(first):
        start = group_rows(first)
        part = blocks // 2
        count = 2 * (2 * rc // tile)

        def place(i):
            row = lax.div(i, 2) * tile
            at = pl.ds(pl.multiple_of(start + row, tile), tile)
            here = pl.ds(pl.multiple_of(lax.rem(row, rc), tile), tile)
            return at, first + lax.div(row, rc), here, lax.rem(i, 2) * part

        def delta_of(spot, b):
            at, group, here, low = spot
            old = wv[at, pl.ds(pl.multiple_of((low + b) * BLOCK, BLOCK), BLOCK)].astype(F32)
            return held[group, low + b, here, :].astype(F32) - old

        def scalings(i):
            spot = place(i)
            found = []
            for b in range(part):
                largest = jnp.max(jnp.abs(delta_of(spot, b)), axis=1, keepdims=True)
                found.append(jnp.broadcast_to((largest + 1e-06) / 7.0, (tile, BLOCK)))
            return tuple(found)

        def body(i, scales):
            spot = place(i)
            ahead = scalings(jnp.minimum(i + 1, count - 1))
            _, group, here, low = spot
            for b in range(part):
                scaling = scales[b]
                offset = offsets[group, low + b, here, :]
                levels = jnp.clip(delta_of(spot, b) * (1.0 / scaling) + offset, -8.0, 7.0)
                smooth = levels - sine_share(levels)
                coded[group, low + b, here, :] = (scaling * (smooth - offset)).astype(BF16)
            return ahead

        lax.fori_loop(0, count, body, scalings(0))

    def merge_groups(first):
        start = group_rows(first)

        @pl.loop(0, 2 * rc // tile)
        def _(i):
            at = pl.multiple_of(start + i * tile, tile)
            group = first + lax.div(i, rc // tile)
            here = pl.ds(pl.multiple_of(lax.rem(i, rc // tile) * tile, tile), tile)
            for b in range(blocks):
                span = slice(b * BLOCK, (b + 1) * BLOCK)
                old = wv[pl.ds(at, tile), span].astype(F32)
                new = fresh[group, b, here, :].astype(F32)
                new_local[pl.ds(at, tile), span] = (mix_share * old + (1.0 - mix_share) * new).astype(BF16)


    def add_into(target, source):
        step = 64 if rc % 64 == 0 else rc

        @pl.loop(0, source.shape[0] * (rc // step))
        def _(i):
            at = (lax.div(i, rc // step), pl.ds(pl.multiple_of(lax.rem(i, rc // step) * step, step), step))
            target[at] = (target[at].astype(F32) + source[at].astype(F32)).astype(BF16)

    def chunk(k):
        g, other = first_group(c, k), first_group(1 - c, k)
        yield from gather(held, k, anchors[k], lambda: code_groups(g))
        code_groups(other)
        got = remote(coded.at[pl.ds(other, 2)], paired.at[k], partner)
        yield
        got.wait_recv()
        ga, gb = g, g + 1

        def spot(group, first, count):
            return coded.at[group, pl.ds(first, count)]

        def take(ab, first, count):
            add_into(spot(g + ab, first, count), paired.at[k, ab, pl.ds(first, count)])

        away = 8 * (1 - pair)
        take(0, away, 8)
        a1 = remote(spot(ga, away, 8), rx1.at[k, 0], {"x": x3})
        take(1, 4 * x1, 4)
        b1 = remote(spot(gb, 4 * x1, 4), rx1.at[k, 1, pl.ds(0, 4)], {"x": x1})
        take(1, 4 * xs[2], 4)
        b2 = remote(spot(gb, 4 * xs[2], 4), rx1.at[k, 1, pl.ds(4, 4)], {"x": x1})
        take(0, 8 * pair, 8)
        take(1, 4 * x, 4)
        take(1, 4 * x3, 4)
        yield
        a1.wait_recv()
        add_into(spot(ga, 4 * x1, 4), rx1.at[k, 0, pl.ds(4 * lax.rem(x1, 2), 4)])
        a3 = remote(spot(ga, 4 * x1, 4), rx2.at[k, 0], {"x": x1})
        b2.wait_recv()
        add_into(spot(gb, 4 * x3, 4), rx1.at[k, 1, pl.ds(4, 4)])
        b3 = remote(spot(gb, 4 * x3, 4), rx2.at[k, 1], {"x": x3})
        add_into(spot(ga, 4 * x, 4), rx1.at[k, 0, pl.ds(4 * lax.rem(x, 2), 4)])
        b1.wait_recv()
        add_into(spot(gb, 4 * x, 4), rx1.at[k, 1, pl.ds(0, 4)])
        yield
        a3.wait_recv()
        add_into(spot(ga, 4 * x, 4), rx2.at[k, 0])
        b3.wait_recv()
        add_into(spot(gb, 4 * x, 4), rx2.at[k, 1])
        over_z = [
            remote(coded.at[pl.ds(g, 2), 4 * x + zs[d]], rz.at[k, d - 1], {"z": zs[d]}) for d in (1, 2, 3)
        ]
        yield
        for copy in over_z:
            copy.wait_recv()
        replicas = 32.0
        for ab in range(2):
            summed = coded[g + ab, mine].astype(F32)
            for d in range(3):
                summed = summed + rz[k, d, ab].astype(F32)
            averaged = summed / replicas
            at = pl.ds((k * 2 + ab) * rc, rc)
            moved = momentum_keep * mom[at] + averaged
            stepped = mas[at] - outer_rate * (averaged + momentum_keep * moved)
            mom[at] = moved
            mas[at] = stepped
            fresh[g + ab, mine] = stepped.astype(BF16)
        news = gather_start(fresh, k)
        span = pl.ds(k * 2 * rc, 2 * rc)
        place = pl.ds(pl.multiple_of(c * half_rows + k * 2 * rc, 2 * rc), 2 * rc)
        theirs = pl.ds(pl.multiple_of((1 - c) * lanes, lanes), lanes)
        back = []
        for which, (values, out) in enumerate(((mas, new_master), (mom, new_momentum))):
            turned[which, :, span] = values[span].T
            back.append(remote(turned.at[which, theirs, span], out.at[:, place], partner))
            out[:, place] = turned[which, my_lanes, span]
        yield from gather(fresh, k, news, lambda: merge_groups(g))
        merge_groups(other)
        yield
        for copy in back:
            copy.wait_recv()

    waiting = []

    def hidden_send(dz, d, first, count):
        here = pl.ds(first, count)
        to_z = (1 - zh) if dz else zh
        span = pl.ds(pl.multiple_of((to_z * 4 + ys[d]) * depth, depth), depth)
        target = {"zh": to_z, "y": ys[d]} if dz else {"y": ys[d]}
        return remote(hidden.at[here, span], hr.at[dz, d, here], target)

    def later(copies, start):
        waiting.append(lambda: copies.append(start()))

    half_columns = columns // 2
    step = 512

    def project(dz, first, count, arrived):
        here = pl.ds(first, count)
        yield
        if dz == 0:
            in_hidden.wait()
        assert len(arrived) == (4 * SUB if dz else 3)
        for copy in arrived:
            copy.wait_recv()

        def products(side, away, stay):
            @pl.loop(0, half_columns // step)
            def _(i):
                at = pl.multiple_of(i * step, step)
                left = hr[dz, :, here].reshape(4 * count, depth)
                right = wv[:, pl.ds(pl.multiple_of(side * half_columns + at, step), step)]
                result = jnp.dot(left, right, preferred_element_type=F32)
                for n in range(2):
                    d = away[n]
                    ps1[dz, side, n, here, pl.ds(at, step)] = result[d * count:(d + 1) * count].astype(BF16)
                    d = stay[n]
                    kept[dz, side, n, here, pl.ds(at, step)] = result[d * count:(d + 1) * count]

        products(0, (1, 2), (0, 3))
        left1 = remote(ps1.at[dz, 0, :, here], pr1.at[dz, 0, :, here], {"y": ys[1]})
        products(1, (2, 3), (0, 1))
        right1 = remote(ps1.at[dz, 1, :, here], pr1.at[dz, 1, :, here], {"y": ys[3]})
        yield
        left1.wait_recv()
        ps2[dz, 0, here] = (kept[dz, 0, 1, here] + pr1[dz, 0, 1, here].astype(F32)).astype(BF16)
        left2 = remote(ps2.at[dz, 0, here], pr2.at[dz, 0, here], {"y": ys[3]})
        yield
        right1.wait_recv()
        ps2[dz, 1, here] = (kept[dz, 1, 1, here] + pr1[dz, 1, 0, here].astype(F32)).astype(BF16)
        right2 = remote(ps2.at[dz, 1, here], pr2.at[dz, 1, here], {"y": ys[1]})
        yield
        left2.wait_recv()
        right2.wait_recv()
        for side in range(2):
            total = kept[dz, side, 0, here] + pr1[dz, side, side, here].astype(F32)
            total = total + pr2[dz, side, here].astype(F32)
            if dz == 1:
                psz[side, here] = total.astype(BF16)
            else:
                kept[dz, side, 0, here] = total
        if dz == 0:
            finished.append("near")
        else:
            crossed = []
            for r in range(RET):
                part = pl.ds(r * (half_columns // RET), half_columns // RET)
                later(crossed, lambda part=part: remote(
                    psz.at[:, here, part], prz.at[:, here, part], {"zh": 1 - zh}))
            yield
            assert len(crossed) == RET
            for copy in crossed:
                copy.wait_recv()
            assert "near" in finished
            for side in range(2):
                total = kept[0, side, 0, here] + prz[side, here].astype(F32)
                key_values[here, side * half_columns:(side + 1) * half_columns] = total.astype(BF16)

    beside = [hidden_send(0, d, 0, tokens) for d in (2, 1, 3)]
    in_master.wait()
    got_master.wait_recv()
    for k in range(NC):
        span = pl.ds(k * 2 * rc, 2 * rc)
        mas[span] = mas_t[:, span].T
        for ab in range(2):
            held[first_group(c, k) + ab, mine] = mas[(k * 2 + ab) * rc:(k * 2 + ab + 1) * rc].astype(BF16)
    anchors = [gather_start(held, k) for k in range(NC)]
    share = tokens // FAR
    crossing = [[] for r in range(FAR)]
    piece = share // SUB
    for r in range(FAR):
        for j in range(SUB):
            for d in (2, 1, 3, 0):
                later(crossing[r], lambda d=d, at=r * share + j * piece: hidden_send(1, d, at, piece))
    in_momentum.wait()
    got_momentum.wait_recv()
    for k in range(NC):
        span = pl.ds(k * 2 * rc, 2 * rc)
        mom[span] = mom_t[:, span].T
    in_dither.wait()
    for k in range(rows // BLOCK):
        span = pl.ds(k * BLOCK, BLOCK)
        narrow[span] = ((dv[:, span].astype(F32) + 0.5) / 16.0 - 0.5).T

    @pl.loop(0, rows // tile)
    def _(i):
        shift = narrow[pl.ds(pl.multiple_of(i * tile, tile), tile), :]
        group = lax.div(i, rc // tile)
        here = pl.ds(pl.multiple_of(lax.rem(i, rc // tile) * tile, tile), tile)
        for b in range(blocks):
            offsets[group, b, here, :] = jnp.broadcast_to(shift[:, b:b + 1], (tile, BLOCK))

    in_weights.wait()

    runs = [chunk(k) for k in range(NC)]
    runs.append(project(0, 0, tokens, beside))
    runs += [project(1, r * share, share, crossing[r]) for r in range(FAR)]
    for run in runs:
        next(run)
    live = list(range(len(runs)))
    for i in ORDER:
        if i < 0:
            waiting.pop(0)()
        elif next(runs[i], "end") == "end":
            live.remove(i)
    assert not live and not waiting
    for copy in sends:
        copy.wait_send()


def shards(hidden, local_weight, master, momentum, dither):
    weights = local_weight[0]
    rows, columns = weights.shape
    tokens, width = hidden.shape
    blocks = columns // BLOCK
    groups = 4 * NC
    rc = rows // groups
    depth = width // 8
    lanes = master.shape[1]
    hbm = pl.BlockSpec(memory_space=pl.ANY)
    vm = pltpu.VMEM
    half = columns // 2
    scratch = [
        vm((rows, columns), BF16),
        vm((blocks, rows), jnp.int32),
        vm((rows, blocks), F32),
        vm((groups, blocks, rc, BLOCK), F32),
        vm((BLOCK, rows // 2), F32),
        vm((BLOCK, rows // 2), F32),
        vm((rows // 2, BLOCK), F32),
        vm((rows // 2, BLOCK), F32),
        vm((2, BLOCK, rows // 2), F32),
        vm((groups, blocks, rc, BLOCK), BF16),
        vm((groups, blocks, rc, BLOCK), BF16),
        vm((NC, 2, blocks, rc, BLOCK), BF16),
        vm((NC, 2, 8, rc, BLOCK), BF16),
        vm((NC, 2, 4, rc, BLOCK), BF16),
        vm((NC, 3, 2, rc, BLOCK), BF16),
        vm((groups, blocks, rc, BLOCK), BF16),
        vm((2, 4, tokens, depth), BF16),
        vm((2, 2, 2, tokens, half), BF16),
        vm((2, 2, 2, tokens, half), BF16),
        vm((2, 2, tokens, half), BF16),
        vm((2, 2, tokens, half), BF16),
        vm((2, tokens, half), BF16),
        vm((2, tokens, half), BF16),
        vm((2, 2, 2, tokens, half), F32),
        pltpu.SemaphoreType.DMA((24 + 42 * NC + (4 + 4 * SUB + RET) * FAR,)),
        pltpu.SemaphoreType.DMA((24 + 42 * NC + (4 + 4 * SUB + RET) * FAR,)),
        pltpu.SemaphoreType.DMA((5,)),
    ]
    key_values, new_master, new_momentum, new_local = pl.pallas_call(
        kernel,
        out_shape=(
            jax.ShapeDtypeStruct((tokens, columns), BF16),
            jax.ShapeDtypeStruct((lanes, rows), F32),
            jax.ShapeDtypeStruct((lanes, rows), F32),
            jax.ShapeDtypeStruct((rows, columns), BF16),
        ),
        in_specs=[hbm] * 5,
        out_specs=[pl.BlockSpec(memory_space=pltpu.VMEM)] * 4,
        scratch_shapes=scratch,
        compiler_params=pltpu.CompilerParams(
            collective_id=0, has_side_effects=True, vmem_limit_bytes=46 * 1024 * 1024
        ),
        name="outer_step",
    )(hidden, weights, dither[0].T, master.T, momentum.T)
    return key_values, new_master.T, new_momentum.T, new_local[None]


def solution(mesh):
    finer = Mesh(mesh.devices.reshape(4, 4, 2, 2, 4), REP_FSDP)
    in_specs = (P(REP_FSDP, None), P(REP, FSDP, None), P(FSDP, REP), P(FSDP, REP), P(REP, FSDP, None))
    out_specs = (P(REP_FSDP, None), P(FSDP, REP), P(FSDP, REP), P(REP, FSDP, None))
    return jax.shard_map(shards, mesh=finer, in_specs=in_specs, out_specs=out_specs, check_vma=False)
```

```python
import functools

import jax
import jax.numpy as jnp
from jax import lax
from jax.experimental import pallas as pl
from jax.experimental.pallas import tpu as pltpu
from jax.sharding import Mesh
from jax.sharding import PartitionSpec as P

BLOCK = 128
FSDP = ("zh", "y")
REP = ("x", "z", "c")
REP_FSDP = ("x", "z", "c", "zh", "y")
MESH = pl.DeviceIdType.MESH

momentum_keep = 0.9
outer_rate = 0.7
mix_share = 0.5

NC = 4
FAR = 2
SUB = 2
RET = 4
ORDER = [-1, 0, 1, -1, 2, 3, 4, -1, 0, 1, -1, 0, 0, -1, 2, 3, 1, 1, -1, 0, -1, 0, -1, 2, 2, 3, 3, 4, 4, -1, 0, 1, -1, 1, -1, 2, -1, 0, 1, 2, -1, 3, 0, 2, 3, -1, 1, 4, 5, 3, -1, 2, 1, 0, 3, 2, 5, 5, 3, 1, 0, 5, 6, -1, 2, -1, 3, 1, 0, 6, 6, -1, 2, 0, 0, -1, 6, 3, 0, 1, -1, 0, 0, -1, 2, 1, 1, -1, 3, 2, 2, 5, -1, 1, 3, 3, 1, 1, 2, 3, 2, 2, 3, 3, 6]
F32 = jnp.float32
BF16 = jnp.bfloat16

SINC = (0.9999999993, -6.579735975, 12.98786004, -12.20766404, 6.688634018, -2.371384249, 0.5153655921)


def sine_share(levels):
    turn = levels - jnp.round(levels)
    square = turn * turn
    series = jnp.full_like(square, SINC[-1])
    for coefficient in SINC[-2::-1]:
        series = series * square + coefficient
    return turn * series


def kernel(
    hidden, weights, dither, master, momentum,
    key_values, new_master, new_momentum, new_local,
    wv, dv, narrow, offsets, mas_t, mom_t, mas, mom, turned,
    held, coded, paired, rx1, rx2, rz, fresh,
    hr, ps1, pr1, ps2, pr2, psz, prz, kept,
    send_sem, recv_sem, local_sem,
):
    rows, columns = wv.shape
    blocks = columns // BLOCK
    lanes = BLOCK // 2
    groups, _, rc, _ = held.shape
    x, z, c = lax.axis_index("x"), lax.axis_index("z"), lax.axis_index("c")
    zh, y = lax.axis_index("zh"), lax.axis_index("y")

    def flips(i):
        return i, i + 1 - 2 * lax.rem(i, 2), lax.rem(i + 2, 4), 3 - i

    xs, zs, ys = flips(x), flips(z), flips(y)
    x1, x3 = xs[1], xs[3]
    mine = x * 4 + z
    pair = lax.div(x, 2)
    partner = {"c": 1 - c}

    counts = {"remote": 0, "local": 0}
    sends = []
    finished = []

    def remote(src, dst, target):
        i = counts["remote"]
        counts["remote"] += 1
        copy = pltpu.make_async_remote_copy(
            src_ref=src, dst_ref=dst, send_sem=send_sem.at[i], recv_sem=recv_sem.at[i],
            device_id=target, device_id_type=MESH,
        )
        copy.start()
        sends.append(copy)
        return copy

    def local(src, dst):
        i = counts["local"]
        counts["local"] += 1
        copy = pltpu.make_async_copy(src, dst, local_sem.at[i])
        copy.start()
        return copy

    half_rows = rows // 2
    my_rows = pl.ds(pl.multiple_of(c * half_rows, half_rows), half_rows)
    other_rows = pl.ds(pl.multiple_of((1 - c) * half_rows, half_rows), half_rows)
    my_lanes = pl.ds(pl.multiple_of(c * lanes, lanes), lanes)
    depth = hr.shape[3]
    tokens = hr.shape[2]
    in_master = local(master.at[:, my_rows], mas_t.at[my_lanes])
    in_dither = local(dither, dv)
    in_weights = local(weights, wv)
    in_momentum = local(momentum.at[:, my_rows], mom_t.at[my_lanes])
    own_columns = pl.ds(pl.multiple_of((zh * 4 + y) * depth, depth), depth)
    in_hidden = local(hidden.at[:, own_columns], hr.at[0, 0])

    barrier = pltpu.get_barrier_semaphore()
    peers = [partner, {"x": x1}, {"x": x3}]
    peers += [{"z": zs[d]} for d in (1, 2, 3)]
    peers += [{"y": ys[d]} for d in (1, 2, 3)]
    peers += [{"zh": 1 - zh, "y": ys[d]} for d in range(4)]
    for peer in peers:
        pl.semaphore_signal(barrier, inc=1, device_id=peer, device_id_type=MESH)
    pl.semaphore_wait(barrier, len(peers))

    got_master = remote(master.at[:, other_rows], mas_t.at[my_lanes], partner)
    got_momentum = remote(momentum.at[:, other_rows], mom_t.at[my_lanes], partner)

    def first_group(half, k):
        return (half * NC + k) * 2

    def group_rows(group):
        return pl.multiple_of(group * rc, rc)

    def gather_start(buffer, k):
        piece = buffer.at[pl.ds(first_group(c, k), 2), mine]
        return [remote(piece, piece, {"z": zs[d]}) for d in (2, 1)]

    def gather(buffer, k, over_z, between=None):
        g = first_group(c, k)

        def pass_on(part):
            return remote(part, part, partner)

        def part(ab, first, count):
            return buffer.at[g + ab, pl.ds(first, count)]

        yield
        far_z, near_z = over_z
        far_z.wait_recv()
        crossed = buffer.at[pl.ds(g, 2), 4 * x + zs[2]]
        onward = remote(crossed, crossed, {"z": zs[1]})
        yield
        near_z.wait_recv()
        onward.wait_recv()
        own_a, own_b = part(0, 4 * x, 4), part(1, 4 * x, 4)
        a1 = remote(own_a, own_a, {"x": x1})
        b1 = remote(own_b, own_b, {"x": x3})
        b2 = remote(own_b, own_b, {"x": x1})
        a2 = remote(own_a, own_a, {"x": x3})
        passed = [pass_on(buffer.at[pl.ds(g, 2), pl.ds(4 * x, 4)])]
        yield
        a1.wait_recv()
        far_a = part(0, 4 * x1, 4)
        a3 = remote(far_a, far_a, {"x": x3})
        passed.append(pass_on(far_a))
        yield
        b1.wait_recv()
        far_b = part(1, 4 * x3, 4)
        b3 = remote(far_b, far_b, {"x": x1})
        passed.append(pass_on(far_b))
        yield
        a2.wait_recv()
        a3.wait_recv()
        passed.append(pass_on(part(0, 8 * (1 - pair), 8)))
        b2.wait_recv()
        passed.append(pass_on(part(1, 4 * x1, 4)))
        b3.wait_recv()
        passed.append(pass_on(part(1, 4 * xs[2], 4)))
        if between is not None:
            between()
        yield
        for copy in passed:
            copy.wait_recv()

    tile = 16

    def code_groups(first):
        start = group_rows(first)
        part = blocks // 2
        count = 2 * (2 * rc // tile)

        def place(i):
            row = lax.div(i, 2) * tile
            at = pl.ds(pl.multiple_of(start + row, tile), tile)
            here = pl.ds(pl.multiple_of(lax.rem(row, rc), tile), tile)
            return at, first + lax.div(row, rc), here, lax.rem(i, 2) * part

        def delta_of(spot, b):
            at, group, here, low = spot
            old = wv[at, pl.ds(pl.multiple_of((low + b) * BLOCK, BLOCK), BLOCK)].astype(F32)
            return held[group, low + b, here, :].astype(F32) - old

        def scalings(i):
            spot = place(i)
            found = []
            for b in range(part):
                largest = jnp.max(jnp.abs(delta_of(spot, b)), axis=1, keepdims=True)
                found.append(jnp.broadcast_to((largest + 1e-06) / 7.0, (tile, BLOCK)))
            return tuple(found)

        def body(i, scales):
            spot = place(i)
            ahead = scalings(jnp.minimum(i + 1, count - 1))
            _, group, here, low = spot
            for b in range(part):
                scaling = scales[b]
                offset = offsets[group, low + b, here, :]
                levels = jnp.clip(delta_of(spot, b) * (1.0 / scaling) + offset, -8.0, 7.0)
                smooth = levels - sine_share(levels)
                coded[group, low + b, here, :] = (scaling * (smooth - offset)).astype(BF16)
            return ahead

        lax.fori_loop(0, count, body, scalings(0))

    def merge_groups(first):
        start = group_rows(first)

        @pl.loop(0, 2 * rc // tile)
        def _(i):
            at = pl.multiple_of(start + i * tile, tile)
            group = first + lax.div(i, rc // tile)
            here = pl.ds(pl.multiple_of(lax.rem(i, rc // tile) * tile, tile), tile)
            for b in range(blocks):
                span = slice(b * BLOCK, (b + 1) * BLOCK)
                old = wv[pl.ds(at, tile), span].astype(F32)
                new = fresh[group, b, here, :].astype(F32)
                new_local[pl.ds(at, tile), span] = (mix_share * old + (1.0 - mix_share) * new).astype(BF16)


    def add_into(target, source):
        step = 64 if rc % 64 == 0 else rc

        @pl.loop(0, source.shape[0] * (rc // step))
        def _(i):
            at = (lax.div(i, rc // step), pl.ds(pl.multiple_of(lax.rem(i, rc // step) * step, step), step))
            target[at] = (target[at].astype(F32) + source[at].astype(F32)).astype(BF16)

    def chunk(k):
        g, other = first_group(c, k), first_group(1 - c, k)
        yield from gather(held, k, anchors[k], lambda: code_groups(g))
        code_groups(other)
        got = remote(coded.at[pl.ds(other, 2)], paired.at[k], partner)
        yield
        got.wait_recv()
        ga, gb = g, g + 1

        def spot(group, first, count):
            return coded.at[group, pl.ds(first, count)]

        def take(ab, first, count):
            add_into(spot(g + ab, first, count), paired.at[k, ab, pl.ds(first, count)])

        away = 8 * (1 - pair)
        take(0, away, 8)
        a1 = remote(spot(ga, away, 8), rx1.at[k, 0], {"x": x3})
        take(1, 4 * x1, 4)
        b1 = remote(spot(gb, 4 * x1, 4), rx1.at[k, 1, pl.ds(0, 4)], {"x": x1})
        take(1, 4 * xs[2], 4)
        b2 = remote(spot(gb, 4 * xs[2], 4), rx1.at[k, 1, pl.ds(4, 4)], {"x": x1})
        take(0, 8 * pair, 8)
        take(1, 4 * x, 4)
        take(1, 4 * x3, 4)
        yield
        a1.wait_recv()
        add_into(spot(ga, 4 * x1, 4), rx1.at[k, 0, pl.ds(4 * lax.rem(x1, 2), 4)])
        a3 = remote(spot(ga, 4 * x1, 4), rx2.at[k, 0], {"x": x1})
        b2.wait_recv()
        add_into(spot(gb, 4 * x3, 4), rx1.at[k, 1, pl.ds(4, 4)])
        b3 = remote(spot(gb, 4 * x3, 4), rx2.at[k, 1], {"x": x3})
        add_into(spot(ga, 4 * x, 4), rx1.at[k, 0, pl.ds(4 * lax.rem(x, 2), 4)])
        b1.wait_recv()
        add_into(spot(gb, 4 * x, 4), rx1.at[k, 1, pl.ds(0, 4)])
        yield
        a3.wait_recv()
        add_into(spot(ga, 4 * x, 4), rx2.at[k, 0])
        b3.wait_recv()
        add_into(spot(gb, 4 * x, 4), rx2.at[k, 1])
        over_z = [
            remote(coded.at[pl.ds(g, 2), 4 * x + zs[d]], rz.at[k, d - 1], {"z": zs[d]}) for d in (1, 2, 3)
        ]
        yield
        for copy in over_z:
            copy.wait_recv()
        replicas = 32.0
        for ab in range(2):
            summed = coded[g + ab, mine].astype(F32)
            for d in range(3):
                summed = summed + rz[k, d, ab].astype(F32)
            averaged = summed / replicas
            at = pl.ds((k * 2 + ab) * rc, rc)
            moved = momentum_keep * mom[at] + averaged
            stepped = mas[at] - outer_rate * (averaged + momentum_keep * moved)
            mom[at] = moved
            mas[at] = stepped
            fresh[g + ab, mine] = stepped.astype(BF16)
        news = gather_start(fresh, k)
        span = pl.ds(k * 2 * rc, 2 * rc)
        place = pl.ds(pl.multiple_of(c * half_rows + k * 2 * rc, 2 * rc), 2 * rc)
        theirs = pl.ds(pl.multiple_of((1 - c) * lanes, lanes), lanes)
        back = []
        for which, (values, out) in enumerate(((mas, new_master), (mom, new_momentum))):
            turned[which, :, span] = values[span].T
            back.append(remote(turned.at[which, theirs, span], out.at[:, place], partner))
            out[:, place] = turned[which, my_lanes, span]
        yield from gather(fresh, k, news, lambda: merge_groups(g))
        merge_groups(other)
        yield
        for copy in back:
            copy.wait_recv()

    waiting = []

    def hidden_send(dz, d, first, count):
        here = pl.ds(first, count)
        to_z = (1 - zh) if dz else zh
        span = pl.ds(pl.multiple_of((to_z * 4 + ys[d]) * depth, depth), depth)
        target = {"zh": to_z, "y": ys[d]} if dz else {"y": ys[d]}
        return remote(hidden.at[here, span], hr.at[dz, d, here], target)

    def later(copies, start):
        waiting.append(lambda: copies.append(start()))

    half_columns = columns // 2
    step = 512

    def project(dz, first, count, arrived):
        here = pl.ds(first, count)
        yield
        if dz == 0:
            in_hidden.wait()
        assert len(arrived) == (4 * SUB if dz else 3)
        for copy in arrived:
            copy.wait_recv()

        def products(side, away, stay):
            @pl.loop(0, half_columns // step)
            def _(i):
                at = pl.multiple_of(i * step, step)
                left = hr[dz, :, here].reshape(4 * count, depth)
                right = wv[:, pl.ds(pl.multiple_of(side * half_columns + at, step), step)]
                result = jnp.dot(left, right, preferred_element_type=F32)
                for n in range(2):
                    d = away[n]
                    ps1[dz, side, n, here, pl.ds(at, step)] = result[d * count:(d + 1) * count].astype(BF16)
                    d = stay[n]
                    kept[dz, side, n, here, pl.ds(at, step)] = result[d * count:(d + 1) * count]

        products(0, (1, 2), (0, 3))
        left1 = remote(ps1.at[dz, 0, :, here], pr1.at[dz, 0, :, here], {"y": ys[1]})
        products(1, (2, 3), (0, 1))
        right1 = remote(ps1.at[dz, 1, :, here], pr1.at[dz, 1, :, here], {"y": ys[3]})
        yield
        left1.wait_recv()
        ps2[dz, 0, here] = (kept[dz, 0, 1, here] + pr1[dz, 0, 1, here].astype(F32)).astype(BF16)
        left2 = remote(ps2.at[dz, 0, here], pr2.at[dz, 0, here], {"y": ys[3]})
        yield
        right1.wait_recv()
        ps2[dz, 1, here] = (kept[dz, 1, 1, here] + pr1[dz, 1, 0, here].astype(F32)).astype(BF16)
        right2 = remote(ps2.at[dz, 1, here], pr2.at[dz, 1, here], {"y": ys[1]})
        yield
        left2.wait_recv()
        right2.wait_recv()
        for side in range(2):
            total = kept[dz, side, 0, here] + pr1[dz, side, side, here].astype(F32)
            total = total + pr2[dz, side, here].astype(F32)
            if dz == 1:
                psz[side, here] = total.astype(BF16)
            else:
                kept[dz, side, 0, here] = total
        if dz == 0:
            finished.append("near")
        else:
            crossed = []
            for r in range(RET):
                part = pl.ds(r * (half_columns // RET), half_columns // RET)
                later(crossed, lambda part=part: remote(
                    psz.at[:, here, part], prz.at[:, here, part], {"zh": 1 - zh}))
            yield
            assert len(crossed) == RET
            for copy in crossed:
                copy.wait_recv()
            assert "near" in finished
            for side in range(2):
                total = kept[0, side, 0, here] + prz[side, here].astype(F32)
                key_values[here, side * half_columns:(side + 1) * half_columns] = total.astype(BF16)

    beside = [hidden_send(0, d, 0, tokens) for d in (2, 1, 3)]
    share = tokens // FAR
    crossing = [[] for r in range(FAR)]
    piece = share // SUB
    for r in range(FAR):
        for j in range(SUB):
            for d in (2, 1, 3, 0):
                later(crossing[r], lambda d=d, at=r * share + j * piece: hidden_send(1, d, at, piece))
    for _ in range(1):
        waiting.pop(0)()
    in_master.wait()
    got_master.wait_recv()
    for k in range(NC):
        span = pl.ds(k * 2 * rc, 2 * rc)
        mas[span] = mas_t[:, span].T
        for ab in range(2):
            held[first_group(c, k) + ab, mine] = mas[(k * 2 + ab) * rc:(k * 2 + ab + 1) * rc].astype(BF16)
    anchors = [gather_start(held, k) for k in range(NC)]
    in_momentum.wait()
    got_momentum.wait_recv()
    for k in range(NC):
        span = pl.ds(k * 2 * rc, 2 * rc)
        mom[span] = mom_t[:, span].T
    in_dither.wait()
    for k in range(rows // BLOCK):
        span = pl.ds(k * BLOCK, BLOCK)
        narrow[span] = ((dv[:, span].astype(F32) + 0.5) / 16.0 - 0.5).T

    @pl.loop(0, rows // tile)
    def _(i):
        shift = narrow[pl.ds(pl.multiple_of(i * tile, tile), tile), :]
        group = lax.div(i, rc // tile)
        here = pl.ds(pl.multiple_of(lax.rem(i, rc // tile) * tile, tile), tile)
        for b in range(blocks):
            offsets[group, b, here, :] = jnp.broadcast_to(shift[:, b:b + 1], (tile, BLOCK))

    in_weights.wait()

    runs = [chunk(k) for k in range(NC)]
    runs.append(project(0, 0, tokens, beside))
    runs += [project(1, r * share, share, crossing[r]) for r in range(FAR)]
    for run in runs:
        next(run)
    live = list(range(len(runs)))
    for i in ORDER:
        if i < 0:
            waiting.pop(0)()
        elif next(runs[i], "end") == "end":
            live.remove(i)
    assert not live and not waiting
    for copy in sends:
        copy.wait_send()


def shards(hidden, local_weight, master, momentum, dither):
    weights = local_weight[0]
    rows, columns = weights.shape
    tokens, width = hidden.shape
    blocks = columns // BLOCK
    groups = 4 * NC
    rc = rows // groups
    depth = width // 8
    lanes = master.shape[1]
    hbm = pl.BlockSpec(memory_space=pl.ANY)
    vm = pltpu.VMEM
    half = columns // 2
    scratch = [
        vm((rows, columns), BF16),
        vm((blocks, rows), jnp.int32),
        vm((rows, blocks), F32),
        vm((groups, blocks, rc, BLOCK), F32),
        vm((BLOCK, rows // 2), F32),
        vm((BLOCK, rows // 2), F32),
        vm((rows // 2, BLOCK), F32),
        vm((rows // 2, BLOCK), F32),
        vm((2, BLOCK, rows // 2), F32),
        vm((groups, blocks, rc, BLOCK), BF16),
        vm((groups, blocks, rc, BLOCK), BF16),
        vm((NC, 2, blocks, rc, BLOCK), BF16),
        vm((NC, 2, 8, rc, BLOCK), BF16),
        vm((NC, 2, 4, rc, BLOCK), BF16),
        vm((NC, 3, 2, rc, BLOCK), BF16),
        vm((groups, blocks, rc, BLOCK), BF16),
        vm((2, 4, tokens, depth), BF16),
        vm((2, 2, 2, tokens, half), BF16),
        vm((2, 2, 2, tokens, half), BF16),
        vm((2, 2, tokens, half), BF16),
        vm((2, 2, tokens, half), BF16),
        vm((2, tokens, half), BF16),
        vm((2, tokens, half), BF16),
        vm((2, 2, 2, tokens, half), F32),
        pltpu.SemaphoreType.DMA((24 + 42 * NC + (4 + 4 * SUB + RET) * FAR,)),
        pltpu.SemaphoreType.DMA((24 + 42 * NC + (4 + 4 * SUB + RET) * FAR,)),
        pltpu.SemaphoreType.DMA((5,)),
    ]
    key_values, new_master, new_momentum, new_local = pl.pallas_call(
        kernel,
        out_shape=(
            jax.ShapeDtypeStruct((tokens, columns), BF16),
            jax.ShapeDtypeStruct((lanes, rows), F32),
            jax.ShapeDtypeStruct((lanes, rows), F32),
            jax.ShapeDtypeStruct((rows, columns), BF16),
        ),
        in_specs=[hbm] * 5,
        out_specs=[pl.BlockSpec(memory_space=pltpu.VMEM)] * 4,
        scratch_shapes=scratch,
        compiler_params=pltpu.CompilerParams(
            collective_id=0, has_side_effects=True, vmem_limit_bytes=46 * 1024 * 1024
        ),
        name="outer_step",
    )(*(
        pltpu.with_memory_space_constraint(operand, pltpu.HBM)
        for operand in (hidden, weights, dither[0].T, master.T, momentum.T)
    ))
    return key_values, new_master.T, new_momentum.T, new_local[None]


def solution(mesh):
    finer = Mesh(mesh.devices.reshape(4, 4, 2, 2, 4), REP_FSDP)
    in_specs = (P(REP_FSDP, None), P(REP, FSDP, None), P(FSDP, REP), P(FSDP, REP), P(REP, FSDP, None))
    out_specs = (P(REP_FSDP, None), P(FSDP, REP), P(FSDP, REP), P(REP, FSDP, None))
    return jax.shard_map(shards, mesh=finer, in_specs=in_specs, out_specs=out_specs, check_vma=False)
```

```python
import functools

import jax
import jax.numpy as jnp
from jax import lax
from jax.experimental import pallas as pl
from jax.experimental.pallas import tpu as pltpu
from jax.sharding import Mesh
from jax.sharding import PartitionSpec as P

BLOCK = 128
FSDP = ("zh", "y")
REP = ("x", "z", "c")
REP_FSDP = ("x", "z", "c", "zh", "y")
MESH = pl.DeviceIdType.MESH

momentum_keep = 0.9
outer_rate = 0.7
mix_share = 0.5

NC = 4
FAR = 4
SUB = 1
RET = 2
ORDER = [0, -1, -1, 2, 0, 1, -1, 3, -1, -1, -1, -1, 0, 0, -1, 1, 4, 2, -1, 0, 1, 1, 5, 3, 0, 2, -1, -1, -1, -1, 2, -1, 1, 0, 3, 3, 1, 2, 5, 1, 2, 0, 3, 2, 1, 0, -1, 3, 5, 6, 2, 1, 3, 5, 7, -1, 6, 2, 3, 4, 1, 0, 6, 3, 7, 7, 8, 2, 1, 4, -1, 0, 3, 2, 8, 6, 1, 8, -1, -1, 0, 1, 2, 3, 8, -1, -1, 7, 0, 1, 0, 3, 2, -1, -1, 4, 6, 5, 1, 2, 3, 3, 0, 0, 2, 3, 8, 1, 2, 2, 1, 3, 7, 3, 0]
F32 = jnp.float32
BF16 = jnp.bfloat16

SINC = (0.9999999993, -6.579735975, 12.98786004, -12.20766404, 6.688634018, -2.371384249, 0.5153655921)


def sine_share(levels):
    turn = levels - jnp.round(levels)
    square = turn * turn
    series = jnp.full_like(square, SINC[-1])
    for coefficient in SINC[-2::-1]:
        series = series * square + coefficient
    return turn * series


def kernel(
    hidden, weights, dither, master, momentum,
    key_values, new_master, new_momentum, new_local,
    wv, dv, narrow, offsets, mas_t, mom_t, mas, mom, turned,
    held, coded, paired, rx1, rx2, rz, fresh,
    hr, ps1, pr1, ps2, pr2, psz, prz, kept,
    send_sem, recv_sem, local_sem,
):
    rows, columns = wv.shape
    blocks = columns // BLOCK
    lanes = BLOCK // 2
    groups, _, rc, _ = held.shape
    x, z, c = lax.axis_index("x"), lax.axis_index("z"), lax.axis_index("c")
    zh, y = lax.axis_index("zh"), lax.axis_index("y")

    def flips(i):
        return i, i + 1 - 2 * lax.rem(i, 2), lax.rem(i + 2, 4), 3 - i

    xs, zs, ys = flips(x), flips(z), flips(y)
    x1, x3 = xs[1], xs[3]
    mine = x * 4 + z
    pair = lax.div(x, 2)
    partner = {"c": 1 - c}

    counts = {"remote": 0, "local": 0}
    sends = []
    finished = []

    def remote(src, dst, target):
        i = counts["remote"]
        counts["remote"] += 1
        copy = pltpu.make_async_remote_copy(
            src_ref=src, dst_ref=dst, send_sem=send_sem.at[i], recv_sem=recv_sem.at[i],
            device_id=target, device_id_type=MESH,
        )
        copy.start()
        sends.append(copy)
        return copy

    def local(src, dst):
        i = counts["local"]
        counts["local"] += 1
        copy = pltpu.make_async_copy(src, dst, local_sem.at[i])
        copy.start()
        return copy

    half_rows = rows // 2
    my_rows = pl.ds(pl.multiple_of(c * half_rows, half_rows), half_rows)
    other_rows = pl.ds(pl.multiple_of((1 - c) * half_rows, half_rows), half_rows)
    my_lanes = pl.ds(pl.multiple_of(c * lanes, lanes), lanes)
    depth = hr.shape[3]
    tokens = hr.shape[2]
    in_master = local(master.at[:, my_rows], mas_t.at[my_lanes])
    in_dither = local(dither, dv)
    in_weights = local(weights, wv)
    in_momentum = local(momentum.at[:, my_rows], mom_t.at[my_lanes])
    own_columns = pl.ds(pl.multiple_of((zh * 4 + y) * depth, depth), depth)
    in_hidden = local(hidden.at[:, own_columns], hr.at[0, 0])

    barrier = pltpu.get_barrier_semaphore()
    peers = [partner, {"x": x1}, {"x": x3}]
    peers += [{"z": zs[d]} for d in (1, 2, 3)]
    peers += [{"y": ys[d]} for d in (1, 2, 3)]
    peers += [{"zh": 1 - zh, "y": ys[d]} for d in range(4)]
    for peer in peers:
        pl.semaphore_signal(barrier, inc=1, device_id=peer, device_id_type=MESH)
    pl.semaphore_wait(barrier, len(peers))

    got_master = remote(master.at[:, other_rows], mas_t.at[my_lanes], partner)
    got_momentum = remote(momentum.at[:, other_rows], mom_t.at[my_lanes], partner)

    def first_group(half, k):
        return (half * NC + k) * 2

    def group_rows(group):
        return pl.multiple_of(group * rc, rc)

    def gather_start(buffer, k):
        piece = buffer.at[pl.ds(first_group(c, k), 2), mine]
        return [remote(piece, piece, {"z": zs[d]}) for d in (2, 1)]

    def gather(buffer, k, over_z, early=None, between=None):
        g = first_group(c, k)

        def pass_on(part):
            return remote(part, part, partner)

        def part(ab, first, count):
            return buffer.at[g + ab, pl.ds(first, count)]

        yield
        far_z, near_z = over_z
        far_z.wait_recv()
        crossed = buffer.at[pl.ds(g, 2), 4 * x + zs[2]]
        onward = remote(crossed, crossed, {"z": zs[1]})
        if early is not None:
            early()
        yield
        near_z.wait_recv()
        onward.wait_recv()
        own_a, own_b = part(0, 4 * x, 4), part(1, 4 * x, 4)
        a1 = remote(own_a, own_a, {"x": x1})
        b1 = remote(own_b, own_b, {"x": x3})
        b2 = remote(own_b, own_b, {"x": x1})
        a2 = remote(own_a, own_a, {"x": x3})
        passed = [pass_on(buffer.at[pl.ds(g, 2), pl.ds(4 * x, 4)])]
        yield
        a1.wait_recv()
        far_a = part(0, 4 * x1, 4)
        a3 = remote(far_a, far_a, {"x": x3})
        passed.append(pass_on(far_a))
        yield
        b1.wait_recv()
        far_b = part(1, 4 * x3, 4)
        b3 = remote(far_b, far_b, {"x": x1})
        passed.append(pass_on(far_b))
        yield
        a2.wait_recv()
        a3.wait_recv()
        passed.append(pass_on(part(0, 8 * (1 - pair), 8)))
        b2.wait_recv()
        passed.append(pass_on(part(1, 4 * x1, 4)))
        b3.wait_recv()
        passed.append(pass_on(part(1, 4 * xs[2], 4)))
        if between is not None:
            between()
        yield
        for copy in passed:
            copy.wait_recv()

    tile = 16

    def code_groups(first):
        start = group_rows(first)
        part = blocks // 2
        count = 2 * (2 * rc // tile)

        def place(i):
            row = lax.div(i, 2) * tile
            at = pl.ds(pl.multiple_of(start + row, tile), tile)
            here = pl.ds(pl.multiple_of(lax.rem(row, rc), tile), tile)
            return at, first + lax.div(row, rc), here, lax.rem(i, 2) * part

        def delta_of(spot, b):
            at, group, here, low = spot
            old = wv[at, pl.ds(pl.multiple_of((low + b) * BLOCK, BLOCK), BLOCK)].astype(F32)
            return held[group, low + b, here, :].astype(F32) - old

        def scalings(i):
            spot = place(i)
            found = []
            for b in range(part):
                largest = jnp.max(jnp.abs(delta_of(spot, b)), axis=1, keepdims=True)
                found.append(jnp.broadcast_to((largest + 1e-06) / 7.0, (tile, BLOCK)))
            return tuple(found)

        def body(i, scales):
            spot = place(i)
            ahead = scalings(jnp.minimum(i + 1, count - 1))
            _, group, here, low = spot
            for b in range(part):
                scaling = scales[b]
                offset = offsets[group, low + b, here, :]
                levels = jnp.clip(delta_of(spot, b) * (1.0 / scaling) + offset, -8.0, 7.0)
                smooth = levels - sine_share(levels)
                coded[group, low + b, here, :] = (scaling * (smooth - offset)).astype(BF16)
            return ahead

        lax.fori_loop(0, count, body, scalings(0), unroll=2)

    def spread_offsets(first):
        start = group_rows(first)

        @pl.loop(0, 2 * rc // tile)
        def _(i):
            shift = narrow[pl.ds(pl.multiple_of(start + i * tile, tile), tile), :]
            group = first + lax.div(i, rc // tile)
            here = pl.ds(pl.multiple_of(lax.rem(i, rc // tile) * tile, tile), tile)
            for b in range(blocks):
                offsets[group, b, here, :] = jnp.broadcast_to(shift[:, b:b + 1], (tile, BLOCK))

    def merge_groups(first):
        start = group_rows(first)

        @pl.loop(0, 2 * rc // tile)
        def _(i):
            at = pl.multiple_of(start + i * tile, tile)
            group = first + lax.div(i, rc // tile)
            here = pl.ds(pl.multiple_of(lax.rem(i, rc // tile) * tile, tile), tile)
            for b in range(blocks):
                span = slice(b * BLOCK, (b + 1) * BLOCK)
                old = wv[pl.ds(at, tile), span].astype(F32)
                new = fresh[group, b, here, :].astype(F32)
                new_local[pl.ds(at, tile), span] = (mix_share * old + (1.0 - mix_share) * new).astype(BF16)


    def add_into(target, source):
        step = 64 if rc % 64 == 0 else rc

        @pl.loop(0, source.shape[0] * (rc // step))
        def _(i):
            at = (lax.div(i, rc // step), pl.ds(pl.multiple_of(lax.rem(i, rc // step) * step, step), step))
            target[at] = (target[at].astype(F32) + source[at].astype(F32)).astype(BF16)

    def chunk(k):
        g, other = first_group(c, k), first_group(1 - c, k)
        def spread():
            spread_offsets(g)
            spread_offsets(other)

        yield from gather(held, k, anchors[k], spread, lambda: code_groups(g))
        code_groups(other)
        got = remote(coded.at[pl.ds(other, 2)], paired.at[k], partner)
        yield
        got.wait_recv()
        ga, gb = g, g + 1

        def spot(group, first, count):
            return coded.at[group, pl.ds(first, count)]

        def take(ab, first, count):
            add_into(spot(g + ab, first, count), paired.at[k, ab, pl.ds(first, count)])

        away = 8 * (1 - pair)
        take(0, away, 8)
        a1 = remote(spot(ga, away, 8), rx1.at[k, 0], {"x": x3})
        take(1, 4 * x1, 4)
        b1 = remote(spot(gb, 4 * x1, 4), rx1.at[k, 1, pl.ds(0, 4)], {"x": x1})
        take(1, 4 * xs[2], 4)
        b2 = remote(spot(gb, 4 * xs[2], 4), rx1.at[k, 1, pl.ds(4, 4)], {"x": x1})
        take(0, 8 * pair, 8)
        take(1, 4 * x, 4)
        take(1, 4 * x3, 4)
        yield
        a1.wait_recv()
        add_into(spot(ga, 4 * x1, 4), rx1.at[k, 0, pl.ds(4 * lax.rem(x1, 2), 4)])
        a3 = remote(spot(ga, 4 * x1, 4), rx2.at[k, 0], {"x": x1})
        b2.wait_recv()
        add_into(spot(gb, 4 * x3, 4), rx1.at[k, 1, pl.ds(4, 4)])
        b3 = remote(spot(gb, 4 * x3, 4), rx2.at[k, 1], {"x": x3})
        add_into(spot(ga, 4 * x, 4), rx1.at[k, 0, pl.ds(4 * lax.rem(x, 2), 4)])
        b1.wait_recv()
        add_into(spot(gb, 4 * x, 4), rx1.at[k, 1, pl.ds(0, 4)])
        yield
        a3.wait_recv()
        add_into(spot(ga, 4 * x, 4), rx2.at[k, 0])
        b3.wait_recv()
        add_into(spot(gb, 4 * x, 4), rx2.at[k, 1])
        over_z = [
            remote(coded.at[pl.ds(g, 2), 4 * x + zs[d]], rz.at[k, d - 1], {"z": zs[d]}) for d in (1, 2, 3)
        ]
        yield
        for copy in over_z:
            copy.wait_recv()
        replicas = 32.0
        for ab in range(2):
            summed = coded[g + ab, mine].astype(F32)
            for d in range(3):
                summed = summed + rz[k, d, ab].astype(F32)
            averaged = summed / replicas
            at = pl.ds((k * 2 + ab) * rc, rc)
            moved = momentum_keep * mom[at] + averaged
            stepped = mas[at] - outer_rate * (averaged + momentum_keep * moved)
            mom[at] = moved
            mas[at] = stepped
            fresh[g + ab, mine] = stepped.astype(BF16)
        news = gather_start(fresh, k)
        span = pl.ds(k * 2 * rc, 2 * rc)
        place = pl.ds(pl.multiple_of(c * half_rows + k * 2 * rc, 2 * rc), 2 * rc)
        theirs = pl.ds(pl.multiple_of((1 - c) * lanes, lanes), lanes)
        back = []
        for which, (values, out) in enumerate(((mas, new_master), (mom, new_momentum))):
            turned[which, :, span] = values[span].T
            back.append(remote(turned.at[which, theirs, span], out.at[:, place], partner))
            out[:, place] = turned[which, my_lanes, span]
        yield from gather(fresh, k, news, None, lambda: merge_groups(g))
        merge_groups(other)
        yield
        for copy in back:
            copy.wait_recv()

    waiting = []

    def hidden_send(dz, d, first, count):
        here = pl.ds(first, count)
        to_z = (1 - zh) if dz else zh
        span = pl.ds(pl.multiple_of((to_z * 4 + ys[d]) * depth, depth), depth)
        target = {"zh": to_z, "y": ys[d]} if dz else {"y": ys[d]}
        return remote(hidden.at[here, span], hr.at[dz, d, here], target)

    def later(copies, start):
        waiting.append(lambda: copies.append(start()))

    half_columns = columns // 2
    step = 512

    def project(dz, first, count, arrived):
        here = pl.ds(first, count)
        yield
        if dz == 0:
            in_hidden.wait()
        assert len(arrived) == (4 * SUB if dz else 3)
        for copy in arrived:
            copy.wait_recv()

        def products(side, away, stay):
            @pl.loop(0, half_columns // step)
            def _(i):
                at = pl.multiple_of(i * step, step)
                left = hr[dz, :, here].reshape(4 * count, depth)
                right = wv[:, pl.ds(pl.multiple_of(side * half_columns + at, step), step)]
                result = jnp.dot(left, right, preferred_element_type=F32)
                for n in range(2):
                    d = away[n]
                    ps1[dz, side, n, here, pl.ds(at, step)] = result[d * count:(d + 1) * count].astype(BF16)
                    d = stay[n]
                    kept[dz, side, n, here, pl.ds(at, step)] = result[d * count:(d + 1) * count]

        products(0, (1, 2), (0, 3))
        left1 = remote(ps1.at[dz, 0, :, here], pr1.at[dz, 0, :, here], {"y": ys[1]})
        products(1, (2, 3), (0, 1))
        right1 = remote(ps1.at[dz, 1, :, here], pr1.at[dz, 1, :, here], {"y": ys[3]})
        yield
        left1.wait_recv()
        ps2[dz, 0, here] = (kept[dz, 0, 1, here] + pr1[dz, 0, 1, here].astype(F32)).astype(BF16)
        left2 = remote(ps2.at[dz, 0, here], pr2.at[dz, 0, here], {"y": ys[3]})
        yield
        right1.wait_recv()
        ps2[dz, 1, here] = (kept[dz, 1, 1, here] + pr1[dz, 1, 0, here].astype(F32)).astype(BF16)
        right2 = remote(ps2.at[dz, 1, here], pr2.at[dz, 1, here], {"y": ys[1]})
        yield
        left2.wait_recv()
        right2.wait_recv()
        for side in range(2):
            total = kept[dz, side, 0, here] + pr1[dz, side, side, here].astype(F32)
            total = total + pr2[dz, side, here].astype(F32)
            if dz == 1:
                psz[side, here] = total.astype(BF16)
            else:
                kept[dz, side, 0, here] = total
        if dz == 0:
            finished.append("near")
        else:
            crossed = []
            for r in range(RET):
                part = pl.ds(r * (half_columns // RET), half_columns // RET)
                later(crossed, lambda part=part: remote(
                    psz.at[:, here, part], prz.at[:, here, part], {"zh": 1 - zh}))
            yield
            assert len(crossed) == RET
            for copy in crossed:
                copy.wait_recv()
            assert "near" in finished
            for side in range(2):
                total = kept[0, side, 0, here] + prz[side, here].astype(F32)
                key_values[here, side * half_columns:(side + 1) * half_columns] = total.astype(BF16)

    beside = [hidden_send(0, d, 0, tokens) for d in (2, 1, 3)]
    share = tokens // FAR
    crossing = [[] for r in range(FAR)]
    piece = share // SUB
    for r in range(FAR):
        for j in range(SUB):
            for d in (2, 1, 3, 0):
                later(crossing[r], lambda d=d, at=r * share + j * piece: hidden_send(1, d, at, piece))
    for _ in range(1):
        waiting.pop(0)()
    in_master.wait()
    got_master.wait_recv()
    for k in range(NC):
        span = pl.ds(k * 2 * rc, 2 * rc)
        mas[span] = mas_t[:, span].T
        for ab in range(2):
            held[first_group(c, k) + ab, mine] = mas[(k * 2 + ab) * rc:(k * 2 + ab + 1) * rc].astype(BF16)
    anchors = [gather_start(held, k) for k in range(NC)]
    in_momentum.wait()
    got_momentum.wait_recv()
    for k in range(NC):
        span = pl.ds(k * 2 * rc, 2 * rc)
        mom[span] = mom_t[:, span].T
    in_dither.wait()
    for k in range(rows // BLOCK):
        span = pl.ds(k * BLOCK, BLOCK)
        narrow[span] = ((dv[:, span].astype(F32) + 0.5) / 16.0 - 0.5).T

    in_weights.wait()

    runs = [chunk(k) for k in range(NC)]
    runs.append(project(0, 0, tokens, beside))
    runs += [project(1, r * share, share, crossing[r]) for r in range(FAR)]
    for run in runs:
        next(run)
    live = list(range(len(runs)))
    for i in ORDER:
        if i < 0:
            waiting.pop(0)()
        elif next(runs[i], "end") == "end":
            live.remove(i)
    assert not live and not waiting
    for copy in sends:
        copy.wait_send()


def shards(hidden, local_weight, master, momentum, dither):
    weights = local_weight[0]
    rows, columns = weights.shape
    tokens, width = hidden.shape
    blocks = columns // BLOCK
    groups = 4 * NC
    rc = rows // groups
    depth = width // 8
    lanes = master.shape[1]
    hbm = pl.BlockSpec(memory_space=pl.ANY)
    vm = pltpu.VMEM
    half = columns // 2
    scratch = [
        vm((rows, columns), BF16),
        vm((blocks, rows), jnp.int32),
        vm((rows, blocks), F32),
        vm((groups, blocks, rc, BLOCK), F32),
        vm((BLOCK, rows // 2), F32),
        vm((BLOCK, rows // 2), F32),
        vm((rows // 2, BLOCK), F32),
        vm((rows // 2, BLOCK), F32),
        vm((2, BLOCK, rows // 2), F32),
        vm((groups, blocks, rc, BLOCK), BF16),
        vm((groups, blocks, rc, BLOCK), BF16),
        vm((NC, 2, blocks, rc, BLOCK), BF16),
        vm((NC, 2, 8, rc, BLOCK), BF16),
        vm((NC, 2, 4, rc, BLOCK), BF16),
        vm((NC, 3, 2, rc, BLOCK), BF16),
        vm((groups, blocks, rc, BLOCK), BF16),
        vm((2, 4, tokens, depth), BF16),
        vm((2, 2, 2, tokens, half), BF16),
        vm((2, 2, 2, tokens, half), BF16),
        vm((2, 2, tokens, half), BF16),
        vm((2, 2, tokens, half), BF16),
        vm((2, tokens, half), BF16),
        vm((2, tokens, half), BF16),
        vm((2, 2, 2, tokens, half), F32),
        pltpu.SemaphoreType.DMA((24 + 42 * NC + (4 + 4 * SUB + RET) * FAR,)),
        pltpu.SemaphoreType.DMA((24 + 42 * NC + (4 + 4 * SUB + RET) * FAR,)),
        pltpu.SemaphoreType.DMA((5,)),
    ]
    key_values, new_master, new_momentum, new_local = pl.pallas_call(
        kernel,
        out_shape=(
            jax.ShapeDtypeStruct((tokens, columns), BF16),
            jax.ShapeDtypeStruct((lanes, rows), F32),
            jax.ShapeDtypeStruct((lanes, rows), F32),
            jax.ShapeDtypeStruct((rows, columns), BF16),
        ),
        in_specs=[hbm] * 5,
        out_specs=[pl.BlockSpec(memory_space=pltpu.VMEM)] * 4,
        scratch_shapes=scratch,
        compiler_params=pltpu.CompilerParams(
            collective_id=0, has_side_effects=True, vmem_limit_bytes=46 * 1024 * 1024
        ),
        name="outer_step",
    )(*(
        pltpu.with_memory_space_constraint(operand, pltpu.HBM)
        for operand in (hidden, weights, dither[0].T, master.T, momentum.T)
    ))
    return key_values, new_master.T, new_momentum.T, new_local[None]


def solution(mesh):
    finer = Mesh(mesh.devices.reshape(4, 4, 2, 2, 4), REP_FSDP)
    in_specs = (P(REP_FSDP, None), P(REP, FSDP, None), P(FSDP, REP), P(FSDP, REP), P(REP, FSDP, None))
    out_specs = (P(REP_FSDP, None), P(FSDP, REP), P(FSDP, REP), P(REP, FSDP, None))
    return jax.shard_map(shards, mesh=finer, in_specs=in_specs, out_specs=out_specs, check_vma=False)
```
